8 devices in a mesh: dp: 1 (over z), depth: 2 (over y), col: 2 (over x), row: 2 (over core).
Axes of the slice: x: 2, y: 2, z: 1, core: 2. Of those that a mesh axis runs over, the one named last changes fastest.
Arguments:
- x_in: bfloat16 [16384, 2048], P(('dp', 'depth', 'row'), 'col')
- ln_gamma: float32 [2048], P('col')
- ln_beta: float32 [2048], P('col')
- w_up: bfloat16 [2048, 8192], P('row', 'col')
- b_up: bfloat16 [8192], P('col')
- w_down: bfloat16 [8192, 2048], P('row', 'col')
- b_down: bfloat16 [2048], P('col')
- grad_out: bfloat16 [16384, 2048], P(('dp', 'depth', 'row'), 'col')
Outputs:
- output 1: bfloat16 [16384, 2048], P(('dp', 'depth', 'row'), 'col')
- output 2: bfloat16 [16384, 2048], P(('dp', 'depth', 'row'), 'col')
- output 3: float32 [2048], P(('dp', 'col'))
- output 4: float32 [2048], P(('dp', 'col'))
- output 5: bfloat16 [2048, 8192], P(('dp', 'row'), 'col')
- output 6: float32 [8192], P(('dp', 'col'))
- output 7: bfloat16 [8192, 2048], P(('dp', 'row'), 'col')
- output 8: float32 [2048], P(('dp', 'col'))
All inputs are finite; a program needn't handle non-finite values.
Results may differ from the reference program's by a relative error of at most 0.0111574.
Values are sent between devices in bfloat16 or wider.
A program may use at most 1 GiB of HBM per device.

```python
import jax
import jax.numpy as jnp
from jax import lax

ROWS = 4096
WIDTH = 2048
FFN = 8192
TOKENS = 16384
SEGMENTS = 64
NUM_BLOCKS = TOKENS // ROWS
SEG_WIDTH = WIDTH // SEGMENTS
LN_EPS = 1e-5


def gelu_tanh(values):
    return jax.nn.gelu(values, approximate=True)


def setup_inputs(seed: int = 0, part: int = 0) -> dict:
    base_key = jax.random.key(seed)
    part_key = jax.random.fold_in(base_key, part)
    key_mean, key_scale, key_noise, key_grad = jax.random.split(part_key, 4)
    shared_key = jax.random.key(seed + 1)
    key_gamma, key_beta, key_wup, key_bup, key_wdown, key_bdown = jax.random.split(shared_key, 6)
    seg_mean = jax.random.normal(key_mean, (TOKENS, SEGMENTS), jnp.float32)
    seg_scale = jax.random.uniform(key_scale, (TOKENS, SEGMENTS), jnp.float32, 0.5, 2.0)
    white_noise = jax.random.normal(key_noise, (TOKENS, WIDTH), jnp.float32)
    x_in = jnp.repeat(seg_mean, SEG_WIDTH, axis=1) + jnp.repeat(seg_scale, SEG_WIDTH, axis=1) * white_noise
    grad_out = jax.random.normal(key_grad, (TOKENS, WIDTH), jnp.float32)
    ln_gamma = jax.random.uniform(key_gamma, (WIDTH,), jnp.float32, 0.5, 1.5)
    ln_beta = 0.5 * jax.random.normal(key_beta, (WIDTH,), jnp.float32)
    w_up = jax.random.normal(key_wup, (WIDTH, FFN), jnp.float32) * WIDTH ** -0.5
    b_up = 0.5 * jax.random.normal(key_bup, (FFN,), jnp.float32)
    w_down = jax.random.normal(key_wdown, (FFN, WIDTH), jnp.float32) * FFN ** -0.5
    b_down = 0.5 * jax.random.normal(key_bdown, (WIDTH,), jnp.float32)
    return {
        'x_in': x_in.astype(jnp.bfloat16),
        'ln_gamma': ln_gamma,
        'ln_beta': ln_beta,
        'w_up': w_up.astype(jnp.bfloat16),
        'b_up': b_up.astype(jnp.bfloat16),
        'w_down': w_down.astype(jnp.bfloat16),
        'b_down': b_down.astype(jnp.bfloat16),
        'grad_out': grad_out.astype(jnp.bfloat16),
    }


def block_pass(x_blk, dy_blk, ln_gamma, ln_beta, w_up, b_up, w_down, b_down):
    x_f32 = x_blk.astype(jnp.float32)
    row_mean = jnp.mean(x_f32, axis=1, keepdims=True)
    centered = x_f32 - row_mean
    row_var = jnp.mean(centered * centered, axis=1, keepdims=True)
    inv_std = lax.rsqrt(row_var + LN_EPS)
    x_hat = centered * inv_std
    x_norm = (x_hat * ln_gamma + ln_beta).astype(jnp.bfloat16)
    pre_act = (jnp.dot(x_norm, w_up, preferred_element_type=jnp.float32) + b_up.astype(jnp.float32)).astype(jnp.bfloat16)
    act_f32, gelu_vjp = jax.vjp(gelu_tanh, pre_act.astype(jnp.float32))
    hidden = act_f32.astype(jnp.bfloat16)
    y_blk = (x_f32 + jnp.dot(hidden, w_down, preferred_element_type=jnp.float32) + b_down.astype(jnp.float32)).astype(jnp.bfloat16)
    dy_f32 = dy_blk.astype(jnp.float32)
    sum_w_down = jnp.dot(hidden.T, dy_blk, preferred_element_type=jnp.float32)
    grad_hidden = jnp.dot(dy_blk, w_down.T, preferred_element_type=jnp.float32)
    grad_pre = gelu_vjp(grad_hidden)[0].astype(jnp.bfloat16)
    sum_w_up = jnp.dot(x_norm.T, grad_pre, preferred_element_type=jnp.float32)
    grad_norm = jnp.dot(grad_pre, w_up.T, preferred_element_type=jnp.float32)
    grad_hat = grad_norm * ln_gamma
    mean_plain = jnp.mean(grad_hat, axis=1, keepdims=True)
    mean_proj = jnp.mean(grad_hat * x_hat, axis=1, keepdims=True)
    dx_blk = (dy_f32 + inv_std * (grad_hat - mean_plain - x_hat * mean_proj)).astype(jnp.bfloat16)
    block_sums = (
        jnp.sum(grad_norm * x_hat, axis=0),
        jnp.sum(grad_norm, axis=0),
        sum_w_up,
        jnp.sum(grad_pre.astype(jnp.float32), axis=0),
        sum_w_down,
        jnp.sum(dy_f32, axis=0),
    )
    return y_blk, dx_blk, block_sums


def reference(x_in, ln_gamma, ln_beta, w_up, b_up, w_down, b_down, grad_out):
    x_blocks = x_in.reshape(NUM_BLOCKS, ROWS, WIDTH)
    dy_blocks = grad_out.reshape(NUM_BLOCKS, ROWS, WIDTH)

    def scan_body(run_sums, blocks):
        y_blk, dx_blk, block_sums = block_pass(blocks[0], blocks[1], ln_gamma, ln_beta, w_up, b_up, w_down, b_down)
        new_sums = jax.tree.map(lambda total, update: total + update, run_sums, block_sums)
        return new_sums, (y_blk, dx_blk)

    init_sums = (
        jnp.zeros((WIDTH,), jnp.float32),
        jnp.zeros((WIDTH,), jnp.float32),
        jnp.zeros((WIDTH, FFN), jnp.float32),
        jnp.zeros((FFN,), jnp.float32),
        jnp.zeros((FFN, WIDTH), jnp.float32),
        jnp.zeros((WIDTH,), jnp.float32),
    )
    final_sums, outputs = lax.scan(scan_body, init_sums, (x_blocks, dy_blocks))
    y_blocks, dx_blocks = outputs
    grad_gamma, grad_beta, sum_w_up, grad_b_up, sum_w_down, grad_b_down = final_sums
    return (
        y_blocks.reshape(TOKENS, WIDTH),
        dx_blocks.reshape(TOKENS, WIDTH),
        grad_gamma,
        grad_beta,
        sum_w_up.astype(jnp.bfloat16),
        grad_b_up,
        sum_w_down.astype(jnp.bfloat16),
        grad_b_down,
    )
```

```python
import jax
import jax.numpy as jnp
from jax import lax
from jax.sharding import PartitionSpec as P


LN_EPS = 1e-5
F32 = jnp.float32
BF16 = jnp.bfloat16
GELU_A = 0.7978845608028654
GELU_B = 0.044715


def gelu_value(v):
    return 0.5 * v * (1.0 + jnp.tanh(GELU_A * (v + GELU_B * (v * v * v))))


def gelu_slope(v):
    sq = v * v
    t = jnp.tanh(GELU_A * (v + GELU_B * (v * sq)))
    return 0.5 * (1.0 + t) + (0.5 * v) * (1.0 - t * t) * (GELU_A + (3.0 * GELU_A * GELU_B) * sq)


def mm(a, b, dims):
    return lax.dot_general(a, b, (dims, ((), ())), preferred_element_type=F32)


NN = ((1,), (0,))
NT = ((1,), (1,))
TN = ((0,), (0,))


def pick(flag, a, b):
    return jnp.where(flag, a, b)


def solution(mesh):
    tok_spec = P(('dp', 'depth', 'row'), 'col')
    vec_spec = P('col')
    mat_spec = P('row', 'col')
    grad_vec = P(('dp', 'col'))
    grad_mat = P(('dp', 'row'), 'col')
    swap = [(0, 1), (1, 0)]

    def local_pass(x, gamma, beta, w_up, b_up, w_down, b_down, dy):
        c = lax.axis_index('col')
        r = lax.axis_index('row')
        d = lax.axis_index('depth')
        rows, half = x.shape
        own = rows // 2
        width = half * 2
        ffn = w_down.shape[0]

        def hop(axis, value, pairs=swap):
            return lax.ppermute(value, axis, pairs)

        def rows_of(value, which, size):
            return lax.dynamic_slice_in_dim(value, which * size, size, 0)

        def cols_of(value, which, size):
            return lax.dynamic_slice_in_dim(value, which * size, size, 1)

        def after(value, *deps):
            return lax.optimization_barrier((value,) + deps)[0]

        def placed(out, axis, parts):
            for index, value in parts:
                out = lax.dynamic_update_slice_in_dim(out, value, index * value.shape[axis], axis)
            return out

        small = jnp.concatenate([gamma, beta, b_up.astype(F32), b_down.astype(F32)])
        small = lax.all_gather(small, 'col', axis=0, tiled=False)
        x, dy, w_up, w_down, small = lax.optimization_barrier((x, dy, w_up, w_down, small))
        peer_vec = lax.dynamic_index_in_dim(small, 1 - c, 0, keepdims=False)
        gam_peer, bet_peer = peer_vec[:half], peer_vec[half:width]
        b_oth = peer_vec[width:width + ffn]
        bd_mine, bd_peer = b_down.astype(F32), peer_vec[width + ffn:]

        x_peer = hop('col', x)
        diag = r == c
        quarter = ffn // 4
        lent = hop(('col', 'row'), rows_of(w_down, (1 - r) * 2 + d, quarter), [(1, 0), (2, 3)])
        d_got = hop('col', pick(diag, lent, rows_of(w_down, r * 2 + d, quarter)))
        dy_peer = hop('col', dy)
        u_got = hop('col', w_up)
        d_rest = hop(('col', 'row'), w_down, [(0, 2), (3, 1)])

        def own_rows(v):
            return rows_of(v, c, own)

        d_mine = lax.all_gather(w_down, 'row', axis=0, tiled=True)
        w_up_c = lax.all_gather(w_up, 'row', axis=0, tiled=True)
        d_peer = lax.all_gather(d_got, ('row', 'depth'), axis=0, tiled=True)
        d_far = lax.all_gather(d_rest, 'row', axis=0, tiled=True)
        w_up_o = lax.all_gather(u_got, 'row', axis=0, tiled=True)
        dm_c, dm_o = rows_of(d_mine, c, ffn), rows_of(d_mine, 1 - c, ffn)
        dp_c, dp_o = d_peer, rows_of(d_far, 1 - c, ffn)

        da_c = lax.optimization_barrier(mm(dy, dm_c, NT))
        da_o = lax.optimization_barrier(mm(own_rows(after(dy, da_c)), dm_o, NT))
        dbd = jnp.sum(dy.astype(F32), axis=0)
        inv_width = 1.0 / width
        sum_mine = lax.optimization_barrier(jnp.sum(x.astype(F32), axis=1, keepdims=True))
        x_peer = after(x_peer, da_o, dbd)
        mu = (sum_mine + jnp.sum(x_peer.astype(F32), axis=1, keepdims=True)) * inv_width

        def square_sum(v):
            cen = v.astype(F32) - mu
            return jnp.sum(cen * cen, axis=1, keepdims=True)

        var = (square_sum(x) + square_sum(x_peer)) * inv_width
        mu, inv = lax.optimization_barrier((mu, lax.rsqrt(var + LN_EPS)))

        def normed(v, g, b):
            return (((v.astype(F32) - mu) * inv) * g + b).astype(BF16)

        xn = placed(jnp.zeros((rows, width), BF16), 1, [(c, normed(x, gamma, beta)), (1 - c, normed(x_peer, gam_peer, bet_peer))])
        xn = after(xn, da_o)

        u_c = (mm(xn, w_up_c, NN) + b_up.astype(F32)).astype(BF16)
        a_c = gelu_value(u_c.astype(F32)).astype(BF16)

        f2, f4 = ffn // 2, ffn // 4
        give = lax.optimization_barrier(mm(cols_of(a_c, 1 - r, f2), dy, TN))
        got = hop('row', give)
        ym_c = lax.optimization_barrier(mm(own_rows(after(a_c, give)), dm_c, NN))
        s = lax.optimization_barrier(mm(cols_of(after(a_c, ym_c), r, f2), dy, TN) + got)
        m_d = lax.optimization_barrier((rows_of(s, d, f4) + hop('depth', rows_of(s, 1 - d, f4))).astype(BF16))

        da_c = da_c + mm(after(dy_peer, s), dp_c, NT)
        du_c = (da_c * gelu_slope(u_c.astype(F32))).astype(BF16)
        dbu = jnp.sum(du_c.astype(F32), axis=0)
        du_c, dbu = lax.optimization_barrier((du_c, dbu))
        m_e = hop('depth', m_d)
        m_got = hop(('col', 'row'), jnp.stack([m_d, m_e]), [(1, 0), (2, 3)])

        e = width // 4
        give = lax.optimization_barrier(mm(cols_of(after(a_c, du_c), 1 - r, f2), dy_peer, TN))
        got = hop('row', give)
        q1 = lax.optimization_barrier(mm(cols_of(after(xn, give), (1 - r) * 2 + (1 - d), e), du_c, TN))
        g1 = hop('row', q1)
        s = lax.optimization_barrier(mm(cols_of(after(a_c, q1), r, f2), dy_peer, TN) + got)
        n_d = lax.optimization_barrier((rows_of(s, d, f4) + hop('depth', rows_of(s, 1 - d, f4))).astype(BF16))
        q2 = lax.optimization_barrier(mm(cols_of(after(xn, s), (1 - r) * 2 + d, e), du_c, TN))
        g2 = hop('row', q2)
        q3 = lax.optimization_barrier(mm(cols_of(after(xn, q2), r * 2 + (1 - d), e), du_c, TN) + g1)
        got = hop('depth', q3)
        q4 = lax.optimization_barrier(mm(cols_of(after(xn, q3), r * 2 + d, e), du_c, TN) + g2)
        dwu_d = lax.optimization_barrier((q4 + got).astype(BF16))
        dwu_e = hop('depth', dwu_d)
        dwu = placed(lax.optimization_barrier(placed(jnp.zeros((half, ffn), BF16), 0, [(d, dwu_d)])), 0, [(1 - d, dwu_e)])

        n_a = hop(('col', 'row'), n_d, [(0, 2), (3, 1)])
        n_b = hop(('col', 'row'), n_d, [(1, 2), (2, 1)])
        n_got = hop(('depth', 'col', 'row'), jnp.stack([n_a, n_b]), [(1, 5), (5, 1), (2, 6), (6, 2)])
        dxn_c = lax.optimization_barrier(mm(own_rows(after(du_c, q4)), w_up_c, NT))
        yp_c = lax.optimization_barrier(mm(own_rows(after(a_c, dxn_c)), dp_c, NN))

        u_o = (mm(own_rows(after(xn, yp_c)), w_up_o, NN) + b_oth).astype(BF16)
        a_o = gelu_value(u_o.astype(F32)).astype(BF16)
        x_own, xr_own = own_rows(x), own_rows(x_peer)
        dy_own, dyr_own = own_rows(dy), own_rows(dy_peer)
        y_give = ((xr_own.astype(F32) + (yp_c + mm(a_o, dp_o, NN))) + bd_peer).astype(BF16)
        y_give = lax.optimization_barrier(y_give)
        y_got = hop('col', y_give)

        da_o = da_o + mm(own_rows(after(dy_peer, y_give)), dp_o, NT)
        du_o = (da_o * gelu_slope(u_o.astype(F32))).astype(BF16)
        du_o = lax.optimization_barrier(du_o)

        mu_o, inv_o = own_rows(mu), own_rows(inv)
        dx_gives, dx_keeps, sums_k = [], [], []
        parts = 2
        n = own // parts
        prev = du_o
        for k in range(parts):
            cut = slice(k * n, (k + 1) * n)
            dxn = dxn_c[cut] + mm(after(du_o, prev)[cut], w_up_o, NT)
            dxn = lax.optimization_barrier(dxn)
            mk, ik = mu_o[cut], inv_o[cut]
            near, far = cols_of(dxn, c, half), cols_of(dxn, 1 - c, half)
            h_near = (x_own[cut].astype(F32) - mk) * ik
            h_far = (xr_own[cut].astype(F32) - mk) * ik
            g_near, g_far = near * gamma, far * gam_peer
            mg = (jnp.sum(g_near, 1, keepdims=True) + jnp.sum(g_far, 1, keepdims=True)) * inv_width
            mp = (jnp.sum(g_near * h_near, 1, keepdims=True) + jnp.sum(g_far * h_far, 1, keepdims=True)) * inv_width
            sums_k.append([jnp.sum(near * h_near, 0), jnp.sum(far * h_far, 0), jnp.sum(near, 0), jnp.sum(far, 0)])
            mg, mp = lax.optimization_barrier((mg, mp))
            dx_far = (dyr_own[cut].astype(F32) + ik * (g_far - mg - h_far * mp)).astype(BF16)
            prev = dx_far = lax.optimization_barrier(dx_far)
            dx_gives.append(hop('col', dx_far))
            dx_keeps.append((dy_own[cut].astype(F32) + ik * (g_near - mg - h_near * mp)).astype(BF16))

        a_l = after(a_o, prev)
        y_keep = ((x_own.astype(F32) + (ym_c + mm(a_l, dm_o, NN))) + bd_mine).astype(BF16)
        y_keep = lax.optimization_barrier(y_keep)
        y_out = lax.optimization_barrier(placed(jnp.zeros((rows, half), BF16), 0, [(c, y_keep), (1 - c, y_got)]))
        dx_out = lax.optimization_barrier(placed(jnp.zeros((rows, half), BF16), 0, [(c * parts + k, dx_keeps[k]) for k in range(parts)]))
        m_d, m_e, m_got, n_a, n_b, n_got = lax.optimization_barrier((m_d, m_e, m_got, n_a, n_b, n_got, y_keep))[:6]
        dwd = placed(jnp.zeros((ffn, half), BF16), 0, [
            (r * 2 + d, pick(diag, m_d, n_a)),
            (r * 2 + 1 - d, pick(diag, m_e, n_got[0])),
            ((1 - r) * 2 + d, pick(diag, m_got[0], n_b)),
            ((1 - r) * 2 + 1 - d, pick(diag, m_got[1], n_got[1])),
        ])

        dwd = lax.optimization_barrier(dwd)
        hn, hf, bn, bf = [a0 + a1 for a0, a1 in zip(*sums_k)]
        at_c = (jnp.arange(2) == c).astype(F32)[:, None]

        def slots(near, far):
            return (at_c * near + (1.0 - at_c) * far).reshape(-1)

        sums = jnp.concatenate([slots(hn, hf), slots(bn, bf), (at_c * dbu).reshape(-1), (at_c * dbd).reshape(-1)])
        sums = lax.psum(after(sums, y_keep, y_out, dx_out, dwd), ('depth', 'col', 'row'))
        dx_out = placed(dx_out, 0, [((1 - c) * parts + k, dx_gives[k]) for k in range(parts)])

        def sums_at(base, size):
            return lax.dynamic_slice_in_dim(sums, base + c * size, size, 0)

        dgam, dbet = sums_at(0, half), sums_at(width, half)
        dbu, dbd = sums_at(2 * width, ffn), sums_at(2 * width + 2 * ffn, half)
        return y_out, dx_out, dgam, dbet, dwu, dbu, dwd, dbd

    return jax.shard_map(
        local_pass,
        mesh=mesh,
        in_specs=(tok_spec, vec_spec, vec_spec, mat_spec, vec_spec, mat_spec, vec_spec, tok_spec),
        out_specs=(tok_spec, tok_spec, grad_vec, grad_vec, grad_mat, grad_vec, grad_mat, grad_vec),
        check_vma=False,
    )
```

```python
import jax
import jax.numpy as jnp
from jax import lax
from jax.sharding import PartitionSpec as P


LN_EPS = 1e-5
F32 = jnp.float32
BF16 = jnp.bfloat16
GELU_A = 0.7978845608028654
GELU_B = 0.044715


def gelu_value(v):
    return 0.5 * v * (1.0 + jnp.tanh(GELU_A * (v + GELU_B * (v * v * v))))


def gelu_slope(v):
    sq = v * v
    t = jnp.tanh(GELU_A * (v + GELU_B * (v * sq)))
    return 0.5 * (1.0 + t) + (0.5 * v) * (1.0 - t * t) * (GELU_A + (3.0 * GELU_A * GELU_B) * sq)


def mm(a, b, dims):
    return lax.dot_general(a, b, (dims, ((), ())), preferred_element_type=F32)


NN = ((1,), (0,))
NT = ((1,), (1,))
TN = ((0,), (0,))


def pick(flag, a, b):
    return jnp.where(flag, a, b)


def solution(mesh):
    tok_spec = P(('dp', 'depth', 'row'), 'col')
    vec_spec = P('col')
    mat_spec = P('row', 'col')
    grad_vec = P(('dp', 'col'))
    grad_mat = P(('dp', 'row'), 'col')
    swap = [(0, 1), (1, 0)]

    def local_pass(x, gamma, beta, w_up, b_up, w_down, b_down, dy):
        c = lax.axis_index('col')
        r = lax.axis_index('row')
        d = lax.axis_index('depth')
        rows, half = x.shape
        own = rows // 2
        width = half * 2
        ffn = w_down.shape[0]

        def hop(axis, value, pairs=swap):
            return lax.ppermute(value, axis, pairs)

        def rows_of(value, which, size):
            return lax.dynamic_slice_in_dim(value, which * size, size, 0)

        def cols_of(value, which, size):
            return lax.dynamic_slice_in_dim(value, which * size, size, 1)

        def after(value, *deps):
            return lax.optimization_barrier((value,) + deps)[0]

        def placed(out, axis, parts):
            for index, value in parts:
                out = lax.dynamic_update_slice_in_dim(out, value, index * value.shape[axis], axis)
            return out

        small = jnp.concatenate([gamma, beta, b_up.astype(F32), b_down.astype(F32)])
        small = lax.all_gather(small, 'col', axis=0, tiled=False)
        x, dy, w_up, w_down, small = lax.optimization_barrier((x, dy, w_up, w_down, small))
        peer_vec = lax.dynamic_index_in_dim(small, 1 - c, 0, keepdims=False)
        gam_peer, bet_peer = peer_vec[:half], peer_vec[half:width]
        b_oth = peer_vec[width:width + ffn]
        bd_mine, bd_peer = b_down.astype(F32), peer_vec[width + ffn:]

        x_peer = hop('col', x)
        diag = r == c
        quarter = ffn // 4
        lent = hop(('col', 'row'), rows_of(w_down, (1 - r) * 2 + d, quarter), [(1, 0), (2, 3)])
        d_got = hop('col', pick(diag, lent, rows_of(w_down, r * 2 + d, quarter)))
        dy_peer = hop('col', dy)
        u_got = hop('col', w_up)
        d_rest = hop(('col', 'row'), w_down, [(0, 2), (3, 1)])

        shapes = ((rows, half), (rows, half), (ffn, half), (half, ffn), (rows, width))
        y_base, dx_base, dwd_base, dwu_base, xn_base = [jnp.full(shape, k, BF16) for k, shape in enumerate(shapes)]

        def own_rows(v):
            return rows_of(v, c, own)

        d_mine = lax.all_gather(w_down, 'row', axis=0, tiled=True)
        w_up_c = lax.all_gather(w_up, 'row', axis=0, tiled=True)
        d_peer = lax.all_gather(d_got, ('row', 'depth'), axis=0, tiled=True)
        d_far = lax.all_gather(d_rest, 'row', axis=0, tiled=True)
        w_up_o = lax.all_gather(u_got, 'row', axis=0, tiled=True)
        dm_c, dm_o = rows_of(d_mine, c, ffn), rows_of(d_mine, 1 - c, ffn)
        dp_c, dp_o = d_peer, rows_of(d_far, 1 - c, ffn)

        da_c = lax.optimization_barrier(mm(dy, dm_c, NT))
        da_o = lax.optimization_barrier(mm(own_rows(after(dy, da_c)), dm_o, NT))
        dbd = jnp.sum(dy.astype(F32), axis=0)
        inv_width = 1.0 / width
        sum_mine = lax.optimization_barrier(jnp.sum(x.astype(F32), axis=1, keepdims=True))
        x_peer = after(x_peer, da_o, dbd)
        mu = (sum_mine + jnp.sum(x_peer.astype(F32), axis=1, keepdims=True)) * inv_width

        def square_sum(v):
            cen = v.astype(F32) - mu
            return jnp.sum(cen * cen, axis=1, keepdims=True)

        var = (square_sum(x) + square_sum(x_peer)) * inv_width
        mu, inv = lax.optimization_barrier((mu, lax.rsqrt(var + LN_EPS)))

        def normed(v, g, b):
            return (((v.astype(F32) - mu) * inv) * g + b).astype(BF16)

        xn = placed(xn_base, 1, [(c, normed(x, gamma, beta)), (1 - c, normed(x_peer, gam_peer, bet_peer))])
        xn = after(xn, da_o)

        u_c = (mm(xn, w_up_c, NN) + b_up.astype(F32)).astype(BF16)
        a_c = gelu_value(u_c.astype(F32)).astype(BF16)

        f2, f4 = ffn // 2, ffn // 4
        give = lax.optimization_barrier(mm(cols_of(a_c, 1 - r, f2), dy, TN))
        got = hop('row', give)
        ym_c = lax.optimization_barrier(mm(own_rows(after(a_c, give)), dm_c, NN))
        s = lax.optimization_barrier(mm(cols_of(after(a_c, ym_c), r, f2), dy, TN) + got)
        m_d = lax.optimization_barrier((rows_of(s, d, f4) + hop('depth', rows_of(s, 1 - d, f4))).astype(BF16))

        da_c = da_c + mm(after(dy_peer, s), dp_c, NT)
        du_c = (da_c * gelu_slope(u_c.astype(F32))).astype(BF16)
        dbu = jnp.sum(du_c.astype(F32), axis=0)
        du_c, dbu = lax.optimization_barrier((du_c, dbu))
        m_e = hop('depth', m_d)
        m_got = [hop(('col', 'row'), v, [(1, 0), (2, 3)]) for v in (m_d, m_e)]

        e = width // 4
        give = lax.optimization_barrier(mm(cols_of(after(a_c, du_c), 1 - r, f2), dy_peer, TN))
        got = hop('row', give)
        q1 = lax.optimization_barrier(mm(cols_of(after(xn, give), (1 - r) * 2 + (1 - d), e), du_c, TN))
        g1 = hop('row', q1)
        s = lax.optimization_barrier(mm(cols_of(after(a_c, q1), r, f2), dy_peer, TN) + got)
        n_d = lax.optimization_barrier((rows_of(s, d, f4) + hop('depth', rows_of(s, 1 - d, f4))).astype(BF16))
        q2 = lax.optimization_barrier(mm(cols_of(after(xn, s), (1 - r) * 2 + d, e), du_c, TN))
        g2 = hop('row', q2)
        q3 = lax.optimization_barrier(mm(cols_of(after(xn, q2), r * 2 + (1 - d), e), du_c, TN) + g1)
        got = hop('depth', q3)
        q4 = lax.optimization_barrier(mm(cols_of(after(xn, q3), r * 2 + d, e), du_c, TN) + g2)
        dwu_d = lax.optimization_barrier((q4 + got).astype(BF16))
        dwu_e = hop('depth', dwu_d)

        n_a = hop(('col', 'row'), n_d, [(0, 2), (3, 1)])
        n_b = hop(('col', 'row'), n_d, [(1, 2), (2, 1)])
        n_got = [hop(('depth', 'col', 'row'), v, [(1, 5), (5, 1), (2, 6), (6, 2)]) for v in (n_a, n_b)]
        dxn_c = lax.optimization_barrier(mm(own_rows(after(du_c, q4)), w_up_c, NT))
        yp_c = lax.optimization_barrier(mm(own_rows(after(a_c, dxn_c)), dp_c, NN))

        u_o = (mm(own_rows(after(xn, yp_c)), w_up_o, NN) + b_oth).astype(BF16)
        a_o = gelu_value(u_o.astype(F32)).astype(BF16)
        x_own, xr_own = own_rows(x), own_rows(x_peer)
        dy_own, dyr_own = own_rows(dy), own_rows(dy_peer)
        y_give = ((xr_own.astype(F32) + (yp_c + mm(a_o, dp_o, NN))) + bd_peer).astype(BF16)
        y_give = lax.optimization_barrier(y_give)
        y_got = hop('col', y_give)

        da_o = da_o + mm(own_rows(after(dy_peer, y_give)), dp_o, NT)
        du_o = (da_o * gelu_slope(u_o.astype(F32))).astype(BF16)
        du_o = lax.optimization_barrier(du_o)

        mu_o, inv_o = own_rows(mu), own_rows(inv)
        dx_gives, dx_keeps, sums_k = [], [], []
        parts = 2
        n = own // parts
        prev = du_o
        for k in range(parts):
            cut = slice(k * n, (k + 1) * n)
            dxn = dxn_c[cut] + mm(after(du_o, prev)[cut], w_up_o, NT)
            dxn = lax.optimization_barrier(dxn)
            mk, ik = mu_o[cut], inv_o[cut]
            near, far = cols_of(dxn, c, half), cols_of(dxn, 1 - c, half)
            h_near = (x_own[cut].astype(F32) - mk) * ik
            h_far = (xr_own[cut].astype(F32) - mk) * ik
            g_near, g_far = near * gamma, far * gam_peer
            mg = (jnp.sum(g_near, 1, keepdims=True) + jnp.sum(g_far, 1, keepdims=True)) * inv_width
            mp = (jnp.sum(g_near * h_near, 1, keepdims=True) + jnp.sum(g_far * h_far, 1, keepdims=True)) * inv_width
            sums_k.append([jnp.sum(near * h_near, 0), jnp.sum(far * h_far, 0), jnp.sum(near, 0), jnp.sum(far, 0)])
            mg, mp = lax.optimization_barrier((mg, mp))
            if k == parts - 1:
                hn, hf, bn, bf = [sum(terms[1:], terms[0]) for terms in zip(*sums_k)]
                near_sums = jnp.concatenate([hn, bn])
                far_got = hop('col', jnp.concatenate([hf, bf]))
            dx_far = (dyr_own[cut].astype(F32) + ik * (g_far - mg - h_far * mp)).astype(BF16)
            prev = dx_far = lax.optimization_barrier(dx_far)
            dx_gives.append(hop('col', dx_far))
            dx_keeps.append((dy_own[cut].astype(F32) + ik * (g_near - mg - h_near * mp)).astype(BF16))

        a_l = after(a_o, prev)
        y_keep = ((x_own.astype(F32) + (ym_c + mm(a_l, dm_o, NN))) + bd_mine).astype(BF16)
        y_keep = lax.optimization_barrier(y_keep)
        dwu = lax.optimization_barrier(placed(dwu_base, 0, [(d, after(dwu_d, y_keep))]))
        y_out = lax.optimization_barrier(placed(y_base, 0, [(c, y_keep), (1 - c, y_got)]))
        dx_out = lax.optimization_barrier(placed(dx_base, 0, [(c * parts + k, after(dx_keeps[k], y_keep)) for k in range(parts)]))
        m_d, m_e, m_got, n_a, n_b, n_got = lax.optimization_barrier((m_d, m_e, tuple(m_got), n_a, n_b, tuple(n_got), y_keep))[:6]
        dwd = placed(dwd_base, 0, [
            (r * 2 + d, pick(diag, m_d, n_a)),
            (r * 2 + 1 - d, pick(diag, m_e, n_got[0])),
            ((1 - r) * 2 + d, pick(diag, m_got[0], n_b)),
            ((1 - r) * 2 + 1 - d, pick(diag, m_got[1], n_got[1])),
        ])

        dwd = lax.optimization_barrier(dwd)
        sums = jnp.concatenate([near_sums + far_got, dbu, dbd])
        sums = lax.psum(after(sums, y_keep, y_out, dx_out, dwd, dwu), ('depth', 'row'))
        dwu = placed(dwu, 0, [(1 - d, dwu_e)])
        dx_out = placed(dx_out, 0, [((1 - c) * parts + k, dx_gives[k]) for k in range(parts)])

        dgam, dbet, dbu, dbd = jnp.split(sums, (half, width, width + ffn))
        return y_out, dx_out, dgam, dbet, dwu, dbu, dwd, dbd

    return jax.shard_map(
        local_pass,
        mesh=mesh,
        in_specs=(tok_spec, vec_spec, vec_spec, mat_spec, vec_spec, mat_spec, vec_spec, tok_spec),
        out_specs=(tok_spec, tok_spec, grad_vec, grad_vec, grad_mat, grad_vec, grad_mat, grad_vec),
        check_vma=False,
    )
```
